16 devices in a mesh: dp: 1, tp: 16 (over x, y, z, core).
Axes of the slice: x: 2, y: 2, z: 2, core: 2. Of those that a mesh axis runs over, the one named last changes fastest.
Arguments:
- x: bfloat16 [2048, 12288], P(('dp', 'tp'))
- dy: bfloat16 [2048, 12288], P(('dp', 'tp'))
- gain: bfloat16 [12288], replicated
- wq: bfloat16 [12288, 12288], P(None, 'tp')
- wk: bfloat16 [12288, 12288], P(None, 'tp')
- wv: bfloat16 [12288, 12288], P(None, 'tp')
- wo: bfloat16 [12288, 12288], P('tp')
Outputs:
- output 1: bfloat16 [2048, 12288], P(('dp', 'tp'))
- output 2: float32 [1, 12288], P('dp')
- output 3: bfloat16 [12288, 12288], P('dp', 'tp')
- output 4: bfloat16 [12288, 12288], P('dp', 'tp')
- output 5: bfloat16 [12288, 12288], P('dp', 'tp')
- output 6: bfloat16 [12288, 12288], P(('dp', 'tp'))
All inputs are finite; a program needn't handle non-finite values.
Results may differ from the reference program's by a relative error of at most 0.018.
Values are sent between devices in bfloat16 or wider.
A program may use at most 2 GiB of HBM per device.

```python
import jax
import jax.numpy as jnp
from jax import lax

ROWS = 2048
D = 12288
HEADS = 96
KV_HEADS = 96
HEAD = 128
THETA = 10000


def setup_inputs(seed: int = 0, part: int = 0) -> dict:
    kx, ky, kn, kq, kk, kv, ko = jax.random.split(jax.random.key(seed), 7)

    def weights(key, rows, columns):
        return jax.random.normal(key, (rows, columns), jnp.float32) * rows**-0.5

    drawn = {
        "x": jax.random.normal(jax.random.fold_in(kx, part), (ROWS, D), jnp.float32),
        "dy": jax.random.normal(jax.random.fold_in(ky, part), (ROWS, D), jnp.float32) * ROWS**-0.5,
        "gain": 1 + 0.1 * jax.random.normal(kn, (D,), jnp.float32),
        "wq": 2 * weights(kq, D, HEADS * HEAD),
        "wk": 2 * weights(kk, D, KV_HEADS * HEAD),
        "wv": 4 * weights(kv, D, KV_HEADS * HEAD),
        "wo": weights(ko, HEADS * HEAD, D),
    }
    return {k: v.astype(jnp.bfloat16) for k, v in drawn.items()}


def normed(x, gain):
    wide = x.astype(jnp.float32)
    scale = lax.rsqrt(jnp.mean(wide * wide, -1, keepdims=True) + 1e-6)
    return (wide * scale * gain.astype(jnp.float32)).astype(jnp.bfloat16)


def turned(t, place, theta):
    half = t.shape[-1] // 2
    angle = place.astype(jnp.float32)[:, None] * theta ** (-jnp.arange(half, dtype=jnp.float32) / half)
    cos, sin = jnp.cos(angle)[:, None], jnp.sin(angle)[:, None]
    a, b = t[..., :half].astype(jnp.float32), t[..., half:].astype(jnp.float32)
    return jnp.concatenate([a * cos - b * sin, b * cos + a * sin], -1).astype(jnp.bfloat16)


def matmul(a, w):
    return jnp.dot(a, w, preferred_element_type=jnp.float32).astype(jnp.bfloat16)


def einsum(form, a, b):
    return jnp.einsum(form, a.astype(jnp.float32), b.astype(jnp.float32))


def attention(q, k, v):
    scores = einsum("tgsd,ugd->gstu", q, k) * q.shape[-1] ** -0.5
    token = jnp.arange(q.shape[0])
    scores = jnp.where(token[:, None] >= token, scores, -jnp.inf)
    weights = jax.nn.softmax(scores, -1).astype(jnp.bfloat16)
    return einsum("gstu,ugd->tgsd", weights, v).astype(jnp.bfloat16)


def forward(x, gain, wq, wk, wv, wo):
    rows = x.shape[0]
    a, place = normed(x, gain), jnp.arange(rows)
    k = turned(matmul(a, wk).reshape(rows, -1, HEAD), place, THETA)
    q = turned(matmul(a, wq).reshape(rows, -1, HEAD), place, THETA).reshape(rows, k.shape[1], -1, HEAD)
    v = matmul(a, wv).reshape(rows, -1, HEAD)
    seen = attention(q, k, v).reshape(rows, -1)
    return (x.astype(jnp.float32) + jnp.dot(seen, wo, preferred_element_type=jnp.float32)).astype(jnp.bfloat16)


def reference(x, dy, gain, wq, wk, wv, wo):
    _, back = jax.vjp(forward, x, gain.astype(jnp.float32), wq, wk, wv, wo)
    by_x, by_gain, *by_weights = back(dy)
    return (by_x, by_gain[None], *by_weights)
```

```python
import functools
import jax, jax.numpy as jnp
from jax import lax
from jax.experimental import pallas as pl
from jax.experimental.pallas import tpu as pltpu
from jax.sharding import PartitionSpec as P

MESH = pl.DeviceIdType.MESH
BIG = 63 * 2**20
HEAD = 128
THETA = 10000


def _place():
    me = lax.axis_index("tp")
    return me // 8, me // 4 % 2, me // 2 % 2, me % 2


def _gather(own, full, send, recv, rounds, lag, work, before, iters):
    x, y, z, c = _place()
    me = lax.axis_index("tp")
    to = {"x": me + 8 * (1 - 2 * x), "y": me + 4 * (1 - 2 * y), "z": me + 2 * (1 - 2 * z), "c": me + 1 - 2 * c}
    a = slice(None)
    routes = [("xyz", (a, y, z, c), (a, a, z, c)), ("yzx", (x, a, z, c), (x, a, a, c)), ("zxy", (x, y, a, c), (a, y, a, c))]
    width = own.shape[1] // rounds
    third = width // 3

    barrier = pltpu.get_barrier_semaphore()
    for peer in to.values():
        pl.semaphore_signal(barrier, inc=1, device_id={"tp": peer}, device_id_type=MESH)
    pl.semaphore_wait(barrier, 4)

    def copy(src, dst, r, n, axis):
        return pltpu.make_async_remote_copy(src_ref=src, dst_ref=dst, send_sem=send.at[r, n], recv_sem=recv.at[r, n],
                                            device_id={"tp": to[axis]}, device_id_type=MESH)

    def hop(r, color, leg):
        axes, second, last = routes[color]
        cols = pl.ds(pl.multiple_of(r * width + color * third, 128), third)
        if leg == 0:
            return copy(own.at[:, cols], full.at[x, y, z, c, :, cols], r, color, axes[0])
        part = full.at[(*(second if leg == 1 else last), a, cols)]
        return copy(part, part, r, 3 * leg + color, axes[leg])

    def across(r):
        part = full.at[:, :, :, c, :, pl.ds(pl.multiple_of(r * width, 128), width)]
        return copy(part, part, r, 9, "c")

    def turn(t, _):
        def at(r, do):
            @pl.when((r >= 0) & (r < rounds))
            def _():
                do(r)

        def leg(n):
            def do(r):
                for color in range(3):
                    if n:
                        hop(r, color, n - 1).wait_recv()
                    hop(r, color, n).start()
            return do

        def cross(r):
            for color in range(3):
                hop(r, color, 2).wait_recv()
            across(r).start()

        def ready(r):
            across(r).wait_recv()
            before(r)

        at(t, leg(0))
        at(t - lag, leg(1))
        at(t - 2 * lag, leg(2))
        at(t - 3 * lag, cross)
        at(t - 4 * lag, ready)
        work(t)
        return None

    lax.fori_loop(0, iters, turn, None)

    def drain(r, _):
        for color in range(3):
            for n in range(3):
                hop(r, color, n).wait_send()
        across(r).wait_send()
        return None

    lax.fori_loop(0, rounds, drain, None)


def _project(own, wq, wk, wv, cos, sin, full, q_ref, k_ref, v_ref, a_s, w_s, acc, keep, load, send, recv, *, rounds, lag):
    rows = own.shape[0]
    width = own.shape[1] // rounds
    wide, tokens = wq.shape[1], q_ref.shape[0]
    x, y, z, c = _place()
    mine = pltpu.make_async_copy(own, full.at[x, y, z, c], keep)
    mine.start()
    acc[...] = jnp.zeros_like(acc)
    mine.wait()

    def loads(r):
        s = r % 2
        cols = pl.ds(pl.multiple_of(r * width, 128), width)
        return [pltpu.make_async_copy(full.at[:, :, :, :, :, cols], a_s.at[s], load.at[s, 3])] + [
            pltpu.make_async_copy(w.at[cols, :], w_s.at[s, n], load.at[s, n]) for n, w in enumerate((wq, wk, wv))]

    def before(r):
        for one in loads(r):
            one.start()

    def work(t):
        r = t - 4 * lag - 1

        @pl.when((r >= 0) & (r < rounds))
        def _():
            for one in loads(r):
                one.wait()
            s = r % 2

            a = a_s[s].reshape(tokens, width)
            per = wide // 256

            def tile(i, _):
                n, at = i // per, pl.ds(pl.multiple_of(i % per * 256, 256), 256)
                acc[n, :, at] += jnp.dot(a, w_s[s, n, :, at], preferred_element_type=jnp.float32)
                return None

            lax.fori_loop(0, 3 * per, tile, None)

    _gather(own, full, send, recv, rounds, lag, work, before, rounds + 4 * lag + 1)

    def finish(i, _):
        at = pl.ds(pl.multiple_of(i * 2 * rows, 2 * rows), 2 * rows)
        co, si = cos[at, :], sin[at, :]
        for h in range(wide // 128):
            hs = pl.ds(h * 128, 128)
            for n, out in ((0, q_ref), (1, k_ref)):
                e = acc[n, at, hs].astype(jnp.bfloat16).astype(jnp.float32)
                out[at, hs] = (e * co + pltpu.roll(e, 64, 1) * si).astype(jnp.bfloat16)
            v_ref[at, hs] = acc[2, at, hs].astype(jnp.bfloat16)
        return None

    lax.fori_loop(0, 8, finish, None)


def project(own, wq, wk, wv, cos, sin, rounds=16, lag=2):
    rows, depth = own.shape
    wide = wq.shape[1]
    tokens = 16 * rows
    width = depth // rounds
    anywhere, vmem = pl.BlockSpec(memory_space=pl.ANY), pl.BlockSpec(memory_space=pltpu.VMEM)
    low = jnp.bfloat16
    full, q, k, v = pl.pallas_call(
        functools.partial(_project, rounds=rounds, lag=lag),
        in_specs=[vmem, anywhere, anywhere, anywhere, vmem, vmem],
        out_specs=[anywhere, vmem, vmem, vmem],
        out_shape=[jax.ShapeDtypeStruct((2, 2, 2, 2, rows, depth), low)] + [jax.ShapeDtypeStruct((tokens, wide), low)] * 3,
        scratch_shapes=[pltpu.VMEM((2, 2, 2, 2, 2, rows, width), low), pltpu.VMEM((2, 3, width, wide), low),
                        pltpu.VMEM((3, tokens, wide), jnp.float32), pltpu.SemaphoreType.DMA, pltpu.SemaphoreType.DMA((2, 4)),
                        pltpu.SemaphoreType.DMA((rounds, 10)), pltpu.SemaphoreType.DMA((rounds, 10))],
        compiler_params=pltpu.CompilerParams(collective_id=1, has_side_effects=True, vmem_limit_bytes=BIG),
        cost_estimate=pl.CostEstimate(flops=6 * tokens * depth * wide, transcendentals=0, bytes_accessed=2 * tokens * depth * 2),
        name="project",
    )(own, wq, wk, wv, cos, sin)
    return full.reshape(tokens, depth), q, k, v


NEG = -1e30
HIDDEN = 2 * NEG
LOG2E = 1.4426950408889634


def _dot(a, b, ca, cb):
    return lax.dot_general(a, b, (((ca,), (cb,)), ((), ())), preferred_element_type=jnp.float32)


def _gap(bk, bq):
    return lax.broadcasted_iota(jnp.int32, (bk, bq), 1) - lax.broadcasted_iota(jnp.int32, (bk, bq), 0)


def _attend(q_ref, k_ref, v_ref, o_ref, lse_ref, top_s, mix_s, gap_s, *, scale, bq, bk):
    heads = q_ref.shape[1] // HEAD
    iq = pl.program_id(0)
    e = scale * LOG2E
    cols = [pl.ds(h * HEAD, HEAD) for h in range(heads)]

    @pl.when(iq == 0)
    def _():
        gap_s[...] = _gap(bk, bq)

    top_s[...] = jnp.full_like(top_s, NEG)
    mix_s[...] = jnp.zeros_like(mix_s)
    ones = jnp.ones((8, bk), jnp.bfloat16)

    def block(j, masked):
        here = pl.ds(pl.multiple_of(j * bk, bk), bk)
        scores = [_dot(k_ref[here, h], q_ref[:, h], 1, 1) for h in cols]
        ok = gap_s[...] >= j * bk - iq * bq if masked else None
        weights, keeps = [], []
        for h, s in enumerate(scores):
            if masked:
                s = jnp.where(ok, s, HIDDEN)
            old = top_s[h : h + 1, :]
            top = jnp.maximum(old, s.max(axis=0, keepdims=True))
            top_s[h : h + 1, :] = top
            weights.append(jnp.exp2((s - top) * e).astype(jnp.bfloat16))
            keeps.append(jnp.exp2((old - top) * e))
        for h, (p, keep) in enumerate(zip(weights, keeps)):
            values = jnp.concatenate([v_ref[here, cols[h]].T, ones], axis=0)
            mix_s[h] = mix_s[h] * keep + _dot(values, p, 1, 0)

    whole = lax.div(iq * bq + 1, bk)
    last = lax.div(iq * bq + bq - 1 + bk, bk)
    lax.fori_loop(0, whole, lambda j, _: block(j, False), None)
    lax.fori_loop(whole, last, lambda j, _: block(j, True), None)
    for h in range(heads):
        total = mix_s[h, HEAD : HEAD + 1, :]
        o_ref[:, cols[h]] = (mix_s[h, :HEAD, :] * (1 / total)).T.astype(o_ref.dtype)
        lse_ref[h : h + 1, :] = top_s[h : h + 1, :] * scale + jnp.log(total)


def attend(q, k, v, bq=512, bk=512):
    rows, wide = q.shape
    heads = wide // HEAD
    return pl.pallas_call(
        functools.partial(_attend, scale=HEAD**-0.5, bq=bq, bk=bk),
        grid=(rows // bq,),
        in_specs=[pl.BlockSpec((bq, wide), lambda i: (i, 0)), pl.BlockSpec((rows, wide), lambda i: (0, 0)), pl.BlockSpec((rows, wide), lambda i: (0, 0))],
        out_specs=[pl.BlockSpec((bq, wide), lambda i: (i, 0)), pl.BlockSpec((heads, bq), lambda i: (0, i))],
        out_shape=[jax.ShapeDtypeStruct((rows, wide), q.dtype), jax.ShapeDtypeStruct((heads, rows), jnp.float32)],
        scratch_shapes=[pltpu.VMEM((heads, bq), jnp.float32), pltpu.VMEM((heads, HEAD + 8, bq), jnp.float32), pltpu.VMEM((bk, bq), jnp.int32)],
        compiler_params=pltpu.CompilerParams(dimension_semantics=("arbitrary",), vmem_limit_bytes=56 * 2**20),
        cost_estimate=pl.CostEstimate(flops=2 * rows * rows * wide, transcendentals=heads * rows * rows // 2, bytes_accessed=8 * rows * wide),
        name="attend",
    )(q, k, v)


def _attend_back(q_ref, k_ref, v_ref, do_ref, out_ref, lse_ref, cos, sin, dq_ref, dk_ref, dv_ref, dq_s, dk_s, dv_s, gap_s, *, scale, bq, bk):
    heads = q_ref.shape[1] // HEAD
    iq = pl.program_id(1)
    e = scale * LOG2E
    cols = [pl.ds(h * HEAD, HEAD) for h in range(heads)]

    @pl.when(iq == 0)
    def _():
        gap_s[...] = _gap(bk, bq)
        dk_s[...] = jnp.zeros_like(dk_s)
        dv_s[...] = jnp.zeros_like(dv_s)

    dq_s[...] = jnp.zeros_like(dq_s)
    lses = [lse_ref[0, h : h + 1, :] * LOG2E for h in range(heads)]
    deltas = [(do_ref[:, h].astype(jnp.float32) * out_ref[:, h].astype(jnp.float32)).T.sum(axis=0, keepdims=True) for h in cols]

    def block(j, masked):
        here = pl.ds(pl.multiple_of(j * bk, bk), bk)
        scores = [_dot(k_ref[here, h], q_ref[:, h], 1, 1) for h in cols]
        dps = [_dot(v_ref[here, h], do_ref[:, h], 1, 1) for h in cols]
        ok = gap_s[...] >= j * bk - iq * bq if masked else None
        for n, h in enumerate(cols):
            p = jnp.exp2(scores[n] * e - lses[n])
            if masked:
                p = jnp.where(ok, p, 0.0)
            ds = (p * (dps[n] - deltas[n])).astype(jnp.bfloat16)
            dv_s[here, h] += _dot(p.astype(jnp.bfloat16), do_ref[:, h], 1, 0)
            dk_s[here, h] += _dot(ds, q_ref[:, h], 1, 0)
            dq_s[n] += _dot(k_ref[here, h].T, ds, 1, 0)

    def back(g, at):
        return (g * cos[at, :] - pltpu.roll(g, HEAD // 2, 1) * sin[at, :]).astype(jnp.bfloat16)

    whole = lax.div(iq * bq + 1, bk)
    last = lax.div(iq * bq + bq - 1 + bk, bk)
    lax.fori_loop(0, whole, lambda j, _: block(j, False), None)
    lax.fori_loop(whole, last, lambda j, _: block(j, True), None)
    for n, h in enumerate(cols):
        dq_ref[:, h] = back((dq_s[n] * scale).T, pl.ds(pl.multiple_of(iq * bq, bq), bq))

    @pl.when(iq == pl.num_programs(1) - 1)
    def _():
        for h in cols:
            dk_ref[:, h] = back(dk_s[:, h] * scale, slice(None))
            dv_ref[:, h] = dv_s[:, h].astype(jnp.bfloat16)


def attend_back(q, k, v, d_out, out, lse, cos, sin, heads=3, bq=512, bk=512):
    rows, wide = q.shape
    part = heads * HEAD
    some = pl.BlockSpec((bq, part), lambda g, i: (i, g))
    every = pl.BlockSpec((rows, part), lambda g, i: (0, g))
    table = pl.BlockSpec((rows, HEAD), lambda g, i: (0, 0))
    return pl.pallas_call(
        functools.partial(_attend_back, scale=HEAD**-0.5, bq=bq, bk=bk),
        grid=(wide // part, rows // bq),
        in_specs=[some, every, every, some, some, pl.BlockSpec((1, heads, bq), lambda g, i: (g, 0, i)), table, table],
        out_specs=[some, every, every],
        out_shape=[jax.ShapeDtypeStruct((rows, wide), q.dtype)] * 3,
        scratch_shapes=[pltpu.VMEM((heads, HEAD, bq), jnp.float32), pltpu.VMEM((rows, part), jnp.float32), pltpu.VMEM((rows, part), jnp.float32),
                        pltpu.VMEM((bk, bq), jnp.int32)],
        compiler_params=pltpu.CompilerParams(dimension_semantics=("arbitrary", "arbitrary"), vmem_limit_bytes=56 * 2**20),
        cost_estimate=pl.CostEstimate(flops=5 * rows * rows * wide, transcendentals=wide // HEAD * rows * rows // 2, bytes_accessed=18 * rows * wide),
        name="attend_back",
    )(q, k, v, d_out, out, lse.reshape(wide // part, heads, rows), cos, sin)


def _by_states(dq, dk, dv, wq, wk, wv, out, away, came, kept, send, recv, *, tile):
    _, _, _, c = _place()
    other = {"tp": lax.axis_index("tp") + 1 - 2 * c}
    i = pl.program_id(0)
    s = i % 2
    chips, rows, part = tile // dq.shape[2], dq.shape[2], dq.shape[3]

    @pl.when(i == 0)
    def _():
        barrier = pltpu.get_barrier_semaphore()
        pl.semaphore_signal(barrier, inc=1, device_id=other, device_id_type=MESH)
        pl.semaphore_wait(barrier, 1)

    def term(core, n):
        at = pl.ds(pl.multiple_of(n * chips, chips), chips)
        flat = [g[at, core].reshape(tile, part) for g in (dq, dk, dv)]
        return _dot(flat[0], wq[...], 1, 1) + _dot(flat[1], wk[...], 1, 1) + _dot(flat[2], wv[...], 1, 1)

    def theirs(n, _):
        away[s, pl.ds(pl.multiple_of(n * chips, chips), chips)] = term(1 - c, n).astype(jnp.bfloat16).reshape(chips, rows, -1)
        return None

    def mine(n, _):
        total = term(c, n).reshape(chips, rows, -1)
        at = pl.ds(pl.multiple_of(n * chips, chips), chips)
        kept[at] = total
        return None

    steps = dq.shape[0] // chips
    lax.fori_loop(0, steps, theirs, None)
    copy = pltpu.make_async_remote_copy(src_ref=away.at[s], dst_ref=came.at[s], send_sem=send.at[s], recv_sem=recv.at[s],
                                        device_id=other, device_id_type=MESH)
    lax.fori_loop(0, 1, mine, None)
    copy.start()
    lax.fori_loop(1, steps, mine, None)
    copy.wait()
    out[...] = (kept[...] + came[s].astype(jnp.float32)).astype(out.dtype)


def by_states(dq, dk, dv, wq, wk, wv, wide=512, tile=512):
    rows, part = dq.shape
    depth = wq.shape[0]
    split = (8, 2, rows // 16, part)
    whole = pl.BlockSpec(split, lambda i: (0, 0, 0, 0))
    some = pl.BlockSpec((wide, part), lambda i: (i, 0))
    half = (8, rows // 16, wide)
    out = pl.pallas_call(
        functools.partial(_by_states, tile=tile),
        grid=(depth // wide,),
        in_specs=[whole] * 3 + [some] * 3,
        out_specs=pl.BlockSpec(half, lambda i: (0, 0, i)),
        out_shape=jax.ShapeDtypeStruct((8, rows // 16, depth), jnp.bfloat16),
        scratch_shapes=[pltpu.VMEM((2, *half), jnp.bfloat16), pltpu.VMEM((2, *half), jnp.bfloat16), pltpu.VMEM(half, jnp.float32),
                        pltpu.SemaphoreType.DMA((2,)), pltpu.SemaphoreType.DMA((2,))],
        compiler_params=pltpu.CompilerParams(dimension_semantics=("arbitrary",), vmem_limit_bytes=56 * 2**20, collective_id=2, has_side_effects=True),
        cost_estimate=pl.CostEstimate(flops=6 * rows * depth * part, transcendentals=0, bytes_accessed=2 * (rows * depth + 3 * depth * part)),
        name="by_states",
    )(*(g.reshape(split) for g in (dq, dk, dv)), wq, wk, wv)
    return out.reshape(rows // 2, depth)


def tables(rows):
    half = HEAD // 2
    angle = jnp.arange(rows, dtype=jnp.float32)[:, None] * THETA ** (-jnp.arange(half, dtype=jnp.float32) / half)
    cos, sin = jnp.cos(angle), jnp.sin(angle)
    return jnp.concatenate([cos, cos], 1), jnp.concatenate([-sin, sin], 1)


def solution(mesh):
    def step(x, dy, gain, wq, wk, wv, wo):
        depth = x.shape[1]
        wide, gain = x.astype(jnp.float32), gain.astype(jnp.float32)
        scale = lax.rsqrt(jnp.mean(wide * wide, -1, keepdims=True) + 1e-6)
        unit = wide * scale
        cos, sin = tables(16 * x.shape[0])
        all_dy = lax.all_gather(dy, "tp", axis=0, tiled=True)
        states, q, k, v = project((unit * gain).astype(jnp.bfloat16), wq, wk, wv, cos, sin)
        seen, lse = attend(q, k, v)
        d_seen = _dot(all_dy, wo, 1, 1).astype(jnp.bfloat16)
        dq, dk, dv = attend_back(q, k, v, d_seen, seen, lse, cos, sin)
        term = by_states(dq, dk, dv, wq, wk, wv)
        cores = [list(range(n, 16, 2)) for n in range(2)]
        d = lax.psum_scatter(term, "tp", scatter_dimension=0, tiled=True, axis_index_groups=cores).astype(jnp.float32)
        by_weights = [_dot(states, g, 0, 0).astype(jnp.bfloat16) for g in (dq, dk, dv)] + [_dot(seen, all_dy, 0, 0).astype(jnp.bfloat16)]
        by_gain = (d * unit).sum(0, keepdims=True)
        by_gain = lax.all_gather(by_gain, "tp", axis=0, tiled=True).sum(0, keepdims=True)
        d = d * gain
        by_x = dy.astype(jnp.float32) + scale * (d - unit * jnp.mean(d * unit, -1, keepdims=True))
        return (by_x.astype(jnp.bfloat16), by_gain, *by_weights)

    tokens, columns = P(("dp", "tp"), None), P(None, "tp")
    return jax.shard_map(
        step,
        mesh=mesh,
        in_specs=(tokens, tokens, P(None), columns, columns, columns, P("tp", None)),
        out_specs=(tokens, P("dp", None), P("dp", "tp"), P("dp", "tp"), P("dp", "tp"), P(("dp", "tp"), None)),
        check_vma=False,
    )
```

```python
import functools
import jax, jax.numpy as jnp
from jax import lax
from jax.experimental import pallas as pl
from jax.experimental.pallas import tpu as pltpu
from jax.sharding import PartitionSpec as P

MESH = pl.DeviceIdType.MESH
BIG = 63 * 2**20
HEAD = 128
THETA = 10000


def _place():
    me = lax.axis_index("tp")
    return me // 8, me // 4 % 2, me // 2 % 2, me % 2


def _gather(own, full, send, recv, rounds, lag, work, before, iters):
    x, y, z, c = _place()
    me = lax.axis_index("tp")
    to = {"x": me + 8 * (1 - 2 * x), "y": me + 4 * (1 - 2 * y), "z": me + 2 * (1 - 2 * z), "c": me + 1 - 2 * c}
    a = slice(None)
    routes = [("xyz", (a, y, z, c), (a, a, z, c)), ("yzx", (x, a, z, c), (x, a, a, c)), ("zxy", (x, y, a, c), (a, y, a, c))]
    width = own.shape[1] // rounds
    third = width // 3

    barrier = pltpu.get_barrier_semaphore()
    for peer in to.values():
        pl.semaphore_signal(barrier, inc=1, device_id={"tp": peer}, device_id_type=MESH)
    pl.semaphore_wait(barrier, 4)

    def copy(src, dst, r, n, axis):
        return pltpu.make_async_remote_copy(src_ref=src, dst_ref=dst, send_sem=send.at[r, n], recv_sem=recv.at[r, n],
                                            device_id={"tp": to[axis]}, device_id_type=MESH)

    def hop(r, color, leg):
        axes, second, last = routes[color]
        cols = pl.ds(pl.multiple_of(r * width + color * third, 128), third)
        if leg == 0:
            return copy(own.at[:, cols], full.at[x, y, z, c, :, cols], r, color, axes[0])
        part = full.at[(*(second if leg == 1 else last), a, cols)]
        return copy(part, part, r, 3 * leg + color, axes[leg])

    def across(r):
        part = full.at[:, :, :, c, :, pl.ds(pl.multiple_of(r * width, 128), width)]
        return copy(part, part, r, 9, "c")

    def turn(t, _):
        def at(r, do):
            @pl.when((r >= 0) & (r < rounds))
            def _():
                do(r)

        def leg(n):
            def do(r):
                for color in range(3):
                    if n:
                        hop(r, color, n - 1).wait_recv()
                    hop(r, color, n).start()
            return do

        def cross(r):
            for color in range(3):
                hop(r, color, 2).wait_recv()
            across(r).start()

        def ready(r):
            across(r).wait_recv()
            before(r)

        at(t, leg(0))
        at(t - lag, leg(1))
        at(t - 2 * lag, leg(2))
        at(t - 3 * lag, cross)
        at(t - 4 * lag, ready)
        work(t)
        return None

    lax.fori_loop(0, iters, turn, None)

    def drain(r, _):
        for color in range(3):
            for n in range(3):
                hop(r, color, n).wait_send()
        across(r).wait_send()
        return None

    lax.fori_loop(0, rounds, drain, None)


def _project(own, wq, wk, wv, cos, sin, full, q_ref, k_ref, v_ref, a_s, w_s, acc, keep, load, send, recv, *, rounds, lag):
    rows = own.shape[0]
    width = own.shape[1] // rounds
    wide, tokens = wq.shape[1], q_ref.shape[0]
    x, y, z, c = _place()
    mine = pltpu.make_async_copy(own, full.at[x, y, z, c], keep)
    mine.start()
    acc[...] = jnp.zeros_like(acc)
    mine.wait()

    def loads(r):
        s = r % 2
        cols = pl.ds(pl.multiple_of(r * width, 128), width)
        return [pltpu.make_async_copy(full.at[:, :, :, :, :, cols], a_s.at[s], load.at[s, 3])] + [
            pltpu.make_async_copy(w.at[cols, :], w_s.at[s, n], load.at[s, n]) for n, w in enumerate((wq, wk, wv))]

    def before(r):
        for one in loads(r):
            one.start()

    def work(t):
        r = t - 4 * lag - 1

        @pl.when((r >= 0) & (r < rounds))
        def _():
            for one in loads(r):
                one.wait()
            s = r % 2

            a = a_s[s].reshape(tokens, width)
            per = wide // 256

            def tile(i, _):
                n, at = i // per, pl.ds(pl.multiple_of(i % per * 256, 256), 256)
                acc[n, :, at] += jnp.dot(a, w_s[s, n, :, at], preferred_element_type=jnp.float32)
                return None

            lax.fori_loop(0, 3 * per, tile, None)

    _gather(own, full, send, recv, rounds, lag, work, before, rounds + 4 * lag + 1)

    def finish(i, _):
        at = pl.ds(pl.multiple_of(i * 2 * rows, 2 * rows), 2 * rows)
        co, si = cos[at, :], sin[at, :]
        for h in range(wide // 128):
            hs = pl.ds(h * 128, 128)
            for n, out in ((0, q_ref), (1, k_ref)):
                e = acc[n, at, hs].astype(jnp.bfloat16).astype(jnp.float32)
                out[at, hs] = (e * co + pltpu.roll(e, 64, 1) * si).astype(jnp.bfloat16)
            v_ref[at, hs] = acc[2, at, hs].astype(jnp.bfloat16)
        return None

    lax.fori_loop(0, 8, finish, None)


def project(own, wq, wk, wv, cos, sin, rounds=16, lag=2):
    rows, depth = own.shape
    wide = wq.shape[1]
    tokens = 16 * rows
    width = depth // rounds
    anywhere, vmem = pl.BlockSpec(memory_space=pl.ANY), pl.BlockSpec(memory_space=pltpu.VMEM)
    low = jnp.bfloat16
    full, q, k, v = pl.pallas_call(
        functools.partial(_project, rounds=rounds, lag=lag),
        in_specs=[vmem, anywhere, anywhere, anywhere, vmem, vmem],
        out_specs=[anywhere, vmem, vmem, vmem],
        out_shape=[jax.ShapeDtypeStruct((2, 2, 2, 2, rows, depth), low)] + [jax.ShapeDtypeStruct((tokens, wide), low)] * 3,
        scratch_shapes=[pltpu.VMEM((2, 2, 2, 2, 2, rows, width), low), pltpu.VMEM((2, 3, width, wide), low),
                        pltpu.VMEM((3, tokens, wide), jnp.float32), pltpu.SemaphoreType.DMA, pltpu.SemaphoreType.DMA((2, 4)),
                        pltpu.SemaphoreType.DMA((rounds, 10)), pltpu.SemaphoreType.DMA((rounds, 10))],
        compiler_params=pltpu.CompilerParams(collective_id=1, has_side_effects=True, vmem_limit_bytes=BIG),
        cost_estimate=pl.CostEstimate(flops=6 * tokens * depth * wide, transcendentals=0, bytes_accessed=2 * tokens * depth * 2),
        name="project",
    )(own, wq, wk, wv, cos, sin)
    return full.reshape(tokens, depth), q, k, v


NEG = -1e30
HIDDEN = 2 * NEG
LOG2E = 1.4426950408889634


def _dot(a, b, ca, cb):
    return lax.dot_general(a, b, (((ca,), (cb,)), ((), ())), preferred_element_type=jnp.float32)


def _gap(bk, bq):
    return lax.broadcasted_iota(jnp.int32, (bk, bq), 1) - lax.broadcasted_iota(jnp.int32, (bk, bq), 0)


def _attend(q_ref, k_ref, v_ref, o_ref, lse_ref, top_s, mix_s, gap_s, *, scale, bq, bk):
    heads = q_ref.shape[1] // HEAD
    iq = pl.program_id(0)
    e = scale * LOG2E
    cols = [pl.ds(h * HEAD, HEAD) for h in range(heads)]

    @pl.when(iq == 0)
    def _():
        gap_s[...] = _gap(bk, bq)

    top_s[...] = jnp.full_like(top_s, NEG)
    mix_s[...] = jnp.zeros_like(mix_s)
    ones = jnp.ones((8, bk), jnp.bfloat16)

    def block(j, masked):
        here = pl.ds(pl.multiple_of(j * bk, bk), bk)
        scores = [_dot(k_ref[here, h], q_ref[:, h], 1, 1) for h in cols]
        ok = gap_s[...] >= j * bk - iq * bq if masked else None
        weights, keeps = [], []
        for h, s in enumerate(scores):
            if masked:
                s = jnp.where(ok, s, HIDDEN)
            old = top_s[h : h + 1, :]
            top = jnp.maximum(old, s.max(axis=0, keepdims=True))
            top_s[h : h + 1, :] = top
            weights.append(jnp.exp2((s - top) * e).astype(jnp.bfloat16))
            keeps.append(jnp.exp2((old - top) * e))
        for h, (p, keep) in enumerate(zip(weights, keeps)):
            values = jnp.concatenate([v_ref[here, cols[h]].T, ones], axis=0)
            mix_s[h] = mix_s[h] * keep + _dot(values, p, 1, 0)

    whole = lax.div(iq * bq + 1, bk)
    last = lax.div(iq * bq + bq - 1 + bk, bk)
    lax.fori_loop(0, whole, lambda j, _: block(j, False), None)
    lax.fori_loop(whole, last, lambda j, _: block(j, True), None)
    for h in range(heads):
        total = mix_s[h, HEAD : HEAD + 1, :]
        o_ref[:, cols[h]] = (mix_s[h, :HEAD, :] * (1 / total)).T.astype(o_ref.dtype)
        lse_ref[h : h + 1, :] = top_s[h : h + 1, :] * scale + jnp.log(total)


def attend(q, k, v, bq=512, bk=512):
    rows, wide = q.shape
    heads = wide // HEAD
    return pl.pallas_call(
        functools.partial(_attend, scale=HEAD**-0.5, bq=bq, bk=bk),
        grid=(rows // bq,),
        in_specs=[pl.BlockSpec((bq, wide), lambda i: (i, 0)), pl.BlockSpec((rows, wide), lambda i: (0, 0)), pl.BlockSpec((rows, wide), lambda i: (0, 0))],
        out_specs=[pl.BlockSpec((bq, wide), lambda i: (i, 0)), pl.BlockSpec((heads, bq), lambda i: (0, i))],
        out_shape=[jax.ShapeDtypeStruct((rows, wide), q.dtype), jax.ShapeDtypeStruct((heads, rows), jnp.float32)],
        scratch_shapes=[pltpu.VMEM((heads, bq), jnp.float32), pltpu.VMEM((heads, HEAD + 8, bq), jnp.float32), pltpu.VMEM((bk, bq), jnp.int32)],
        compiler_params=pltpu.CompilerParams(dimension_semantics=("arbitrary",), vmem_limit_bytes=56 * 2**20),
        cost_estimate=pl.CostEstimate(flops=2 * rows * rows * wide, transcendentals=heads * rows * rows // 2, bytes_accessed=8 * rows * wide),
        name="attend",
    )(q, k, v)


def _attend_back(q_ref, k_ref, v_ref, do_ref, out_ref, lse_ref, cos, sin, dq_ref, dk_ref, dv_ref, dq_s, dk_s, dv_s, gap_s, *, scale, bq, bk):
    heads = q_ref.shape[1] // HEAD
    iq = pl.program_id(1)
    e = scale * LOG2E
    cols = [pl.ds(h * HEAD, HEAD) for h in range(heads)]

    @pl.when(iq == 0)
    def _():
        gap_s[...] = _gap(bk, bq)
        dk_s[...] = jnp.zeros_like(dk_s)
        dv_s[...] = jnp.zeros_like(dv_s)

    dq_s[...] = jnp.zeros_like(dq_s)
    lses = [lse_ref[0, h : h + 1, :] * LOG2E for h in range(heads)]
    deltas = [(do_ref[:, h].astype(jnp.float32) * out_ref[:, h].astype(jnp.float32)).T.sum(axis=0, keepdims=True) for h in cols]

    def block(j, masked):
        here = pl.ds(pl.multiple_of(j * bk, bk), bk)
        scores = [_dot(k_ref[here, h], q_ref[:, h], 1, 1) for h in cols]
        dps = [_dot(v_ref[here, h], do_ref[:, h], 1, 1) for h in cols]
        ok = gap_s[...] >= j * bk - iq * bq if masked else None
        for n, h in enumerate(cols):
            p = jnp.exp2(scores[n] * e - lses[n])
            if masked:
                p = jnp.where(ok, p, 0.0)
            ds = (p * (dps[n] - deltas[n])).astype(jnp.bfloat16)
            dv_s[here, h] += _dot(p.astype(jnp.bfloat16), do_ref[:, h], 1, 0)
            dk_s[here, h] += _dot(ds, q_ref[:, h], 1, 0)
            dq_s[n] += _dot(k_ref[here, h].T, ds, 1, 0)

    def back(g, at):
        return (g * cos[at, :] - pltpu.roll(g, HEAD // 2, 1) * sin[at, :]).astype(jnp.bfloat16)

    whole = lax.div(iq * bq + 1, bk)
    last = lax.div(iq * bq + bq - 1 + bk, bk)
    lax.fori_loop(0, whole, lambda j, _: block(j, False), None)
    lax.fori_loop(whole, last, lambda j, _: block(j, True), None)
    for n, h in enumerate(cols):
        dq_ref[:, h] = back((dq_s[n] * scale).T, pl.ds(pl.multiple_of(iq * bq, bq), bq))

    @pl.when(iq == pl.num_programs(1) - 1)
    def _():
        for h in cols:
            dk_ref[:, h] = back(dk_s[:, h] * scale, slice(None))
            dv_ref[:, h] = dv_s[:, h].astype(jnp.bfloat16)


def attend_back(q, k, v, d_out, out, lse, cos, sin, heads=3, bq=512, bk=512):
    rows, wide = q.shape
    part = heads * HEAD
    some = pl.BlockSpec((bq, part), lambda g, i: (i, g))
    every = pl.BlockSpec((rows, part), lambda g, i: (0, g))
    table = pl.BlockSpec((rows, HEAD), lambda g, i: (0, 0))
    return pl.pallas_call(
        functools.partial(_attend_back, scale=HEAD**-0.5, bq=bq, bk=bk),
        grid=(wide // part, rows // bq),
        in_specs=[some, every, every, some, some, pl.BlockSpec((1, heads, bq), lambda g, i: (g, 0, i)), table, table],
        out_specs=[some, every, every],
        out_shape=[jax.ShapeDtypeStruct((rows, wide), q.dtype)] * 3,
        scratch_shapes=[pltpu.VMEM((heads, HEAD, bq), jnp.float32), pltpu.VMEM((rows, part), jnp.float32), pltpu.VMEM((rows, part), jnp.float32),
                        pltpu.VMEM((bk, bq), jnp.int32)],
        compiler_params=pltpu.CompilerParams(dimension_semantics=("arbitrary", "arbitrary"), vmem_limit_bytes=56 * 2**20),
        cost_estimate=pl.CostEstimate(flops=5 * rows * rows * wide, transcendentals=wide // HEAD * rows * rows // 2, bytes_accessed=18 * rows * wide),
        name="attend_back",
    )(q, k, v, d_out, out, lse.reshape(wide // part, heads, rows), cos, sin)


def _by_states(dq, dk, dv, wq, wk, wv, out, away, came, kept, send, recv, *, tile):
    _, _, _, c = _place()
    other = {"tp": lax.axis_index("tp") + 1 - 2 * c}
    i = pl.program_id(0)
    s = i % 2
    chips, rows, part = tile // dq.shape[2], dq.shape[2], dq.shape[3]

    @pl.when(i == 0)
    def _():
        barrier = pltpu.get_barrier_semaphore()
        pl.semaphore_signal(barrier, inc=1, device_id=other, device_id_type=MESH)
        pl.semaphore_wait(barrier, 1)

    def term(core, n):
        at = pl.ds(pl.multiple_of(n * chips, chips), chips)
        flat = [g[at, core].reshape(tile, part) for g in (dq, dk, dv)]
        return _dot(flat[0], wq[...], 1, 1) + _dot(flat[1], wk[...], 1, 1) + _dot(flat[2], wv[...], 1, 1)

    away[s] = term(1 - c, 0).astype(jnp.bfloat16).reshape(chips, rows, -1)
    copy = pltpu.make_async_remote_copy(src_ref=away.at[s], dst_ref=came.at[s], send_sem=send.at[s], recv_sem=recv.at[s],
                                        device_id=other, device_id_type=MESH)
    kept[...] = _dot(dq[:, c].reshape(tile, part), wq[...], 1, 1).reshape(chips, rows, -1)
    copy.start()
    kept[...] += (_dot(dk[:, c].reshape(tile, part), wk[...], 1, 1) + _dot(dv[:, c].reshape(tile, part), wv[...], 1, 1)).reshape(chips, rows, -1)
    copy.wait()
    out[...] = (kept[...] + came[s].astype(jnp.float32)).astype(out.dtype)


def by_states(dq, dk, dv, wq, wk, wv, wide=512, tile=1024):
    rows, part = dq.shape
    depth = wq.shape[0]
    split = (8, 2, rows // 16, part)
    whole = pl.BlockSpec(split, lambda i: (0, 0, 0, 0))
    some = pl.BlockSpec((wide, part), lambda i: (i, 0))
    half = (8, rows // 16, wide)
    out = pl.pallas_call(
        functools.partial(_by_states, tile=tile),
        grid=(depth // wide,),
        in_specs=[whole] * 3 + [some] * 3,
        out_specs=pl.BlockSpec(half, lambda i: (0, 0, i)),
        out_shape=jax.ShapeDtypeStruct((8, rows // 16, depth), jnp.bfloat16),
        scratch_shapes=[pltpu.VMEM((2, *half), jnp.bfloat16), pltpu.VMEM((2, *half), jnp.bfloat16), pltpu.VMEM(half, jnp.float32),
                        pltpu.SemaphoreType.DMA((2,)), pltpu.SemaphoreType.DMA((2,))],
        compiler_params=pltpu.CompilerParams(dimension_semantics=("arbitrary",), vmem_limit_bytes=56 * 2**20, collective_id=2, has_side_effects=True),
        cost_estimate=pl.CostEstimate(flops=6 * rows * depth * part, transcendentals=0, bytes_accessed=2 * (rows * depth + 3 * depth * part)),
        name="by_states",
    )(*(g.reshape(split) for g in (dq, dk, dv)), wq, wk, wv)
    return out.reshape(rows // 2, depth)


def tables(rows):
    half = HEAD // 2
    angle = jnp.arange(rows, dtype=jnp.float32)[:, None] * THETA ** (-jnp.arange(half, dtype=jnp.float32) / half)
    cos, sin = jnp.cos(angle), jnp.sin(angle)
    return jnp.concatenate([cos, cos], 1), jnp.concatenate([-sin, sin], 1)


def solution(mesh):
    def step(x, dy, gain, wq, wk, wv, wo):
        depth = x.shape[1]
        wide, gain = x.astype(jnp.float32), gain.astype(jnp.float32)
        scale = lax.rsqrt(jnp.mean(wide * wide, -1, keepdims=True) + 1e-6)
        unit = wide * scale
        cos, sin = tables(16 * x.shape[0])
        all_dy = lax.all_gather(dy, "tp", axis=0, tiled=True)
        states, q, k, v = project((unit * gain).astype(jnp.bfloat16), wq, wk, wv, cos, sin)
        seen, lse = attend(q, k, v)
        d_seen = _dot(all_dy, wo, 1, 1).astype(jnp.bfloat16)
        dq, dk, dv = attend_back(q, k, v, d_seen, seen, lse, cos, sin)
        term = by_states(dq, dk, dv, wq, wk, wv)
        cores = [list(range(n, 16, 2)) for n in range(2)]
        d = lax.psum_scatter(term, "tp", scatter_dimension=0, tiled=True, axis_index_groups=cores).astype(jnp.float32)
        by_weights = [_dot(states, g, 0, 0).astype(jnp.bfloat16) for g in (dq, dk, dv)] + [_dot(seen, all_dy, 0, 0).astype(jnp.bfloat16)]
        by_gain = (d * unit).sum(0, keepdims=True)
        by_gain = lax.all_gather(by_gain, "tp", axis=0, tiled=True).sum(0, keepdims=True)
        d = d * gain
        by_x = dy.astype(jnp.float32) + scale * (d - unit * jnp.mean(d * unit, -1, keepdims=True))
        return (by_x.astype(jnp.bfloat16), by_gain, *by_weights)

    tokens, columns = P(("dp", "tp"), None), P(None, "tp")
    return jax.shard_map(
        step,
        mesh=mesh,
        in_specs=(tokens, tokens, P(None), columns, columns, columns, P("tp", None)),
        out_specs=(tokens, P("dp", None), P("dp", "tp"), P("dp", "tp"), P("dp", "tp"), P(("dp", "tp"), None)),
        check_vma=False,
    )
```
